32 devices in a mesh: grp: 4 (over y, x), dev: 8 (over z, core).
Axes of the slice: x: 2, y: 2, z: 4, core: 2. Of those that a mesh axis runs over, the one named last changes fastest.
Arguments:
- token_ids: int32 [128, 128], P(('grp', 'dev')), may hold values from 0 to 128255, as said below
- sensitivity: bfloat16 [128, 128, 4096], P(('grp', 'dev')), may hold values from -6 to 6
- last_hidden: bfloat16 [128, 4096], P(('grp', 'dev')), may hold values from -6 to 6
- lengths: int32 [128], P(('grp', 'dev')), may hold values from 97 to 128
- norm_gain: float32 [4096], replicated, may hold values from 0.25 to 1.75
- reward_head: float32 [4096], replicated, may hold values from -0.09375 to 0.09375
- chosen_index: int32 [64], replicated, may hold values from 0 to 127, as said below
- rejected_index: int32 [64], replicated, may hold values from 0 to 127, as said below
- shard_owner: int32 [32], replicated, may hold values from 0 to 31, each once
Outputs:
- owned_grad: bfloat16 [128256, 4096], P(('grp', 'dev'))
- head_grad: float32 [4096], P(('grp', 'dev'))
The draws below stay inside these ranges and needn't reach their ends.
Inputs may be any that keep to these rules, and one draw needn't show every extreme that they name: `token_ids`: within the token slots of one device, at most 32 ids fall in any one vocabulary shard of 4008 rows, and on every device some shard gets exactly 32. chosen_index and rejected_index together name every response exactly once. `rejected_index`: see chosen_index.
All inputs are finite; a program needn't handle non-finite values.
Results may differ from the reference program's by a relative error of at most 0.0042.
Values may be sent and summed in bfloat16 or wider, within the bound.
A program may use at most 128 MiB of HBM per device.

```python
import jax
import jax.numpy as jnp
from jax import lax

D = 4096
VOCAB = 128256
BLOCK = 128
RESP_DEV = 4
TOK_DEV = 512
RESPONSES = 128
PAIRS = 64
SHARD = 4008
CAP = 32
DEVICES = 32


def pair_split(key):
    order = jax.random.permutation(jax.random.fold_in(key, 7), RESPONSES).astype(jnp.int32)
    return (order[:PAIRS], order[PAIRS:])


def draw_chosen_index(key, part):
    return pair_split(key)[0]


def draw_rejected_index(key, part):
    return pair_split(key)[1]


def draw_token_ids(key, part):
    total = DEVICES * CAP

    def one_device(dev_key):
        key_first, key_order, key_shuffle, key_offset = jax.random.split(dev_key, 4)
        labels = jnp.arange(total, dtype=jnp.int32) // CAP
        within = jnp.arange(total, dtype=jnp.int32) % CAP
        first = jax.random.randint(key_first, (), 0, DEVICES, dtype=jnp.int32)
        order = jax.random.permutation(key_order, total).astype(jnp.int32)
        score = jnp.where(labels == first, within - CAP, order)
        picked = jnp.argsort(score, stable=True)[:TOK_DEV]
        shards = jax.random.permutation(key_shuffle, labels[picked])
        offset = jax.random.randint(key_offset, (TOK_DEV,), 0, SHARD, dtype=jnp.int32)
        return (shards * SHARD + offset).astype(jnp.int32)
    keys = jax.random.split(jax.random.fold_in(key, 11), DEVICES)
    return jax.vmap(one_device)(keys).reshape(RESPONSES, BLOCK)


def set_ends(drawn, stream_key, low, top_value):
    longest = drawn.shape.index(max(drawn.shape))
    spots = []
    for shift in (0, 1):
        where = [jax.random.randint(jax.random.fold_in(stream_key, axis), (), 0, length) for axis, length in enumerate(drawn.shape)]
        where[longest] = (where[longest] + shift) % drawn.shape[longest]
        spots.append(tuple(where))
    return drawn.at[spots[0]].set(low).at[spots[1]].set(top_value)


def level_of(own_key, extent, cuts, smallest, largest):
    loudness = 1.0
    for axis_at, parts in cuts:
        draws = jax.random.uniform(jax.random.fold_in(jax.random.fold_in(own_key, 6), axis_at), (parts,), jnp.float32, smallest / len(cuts), largest / len(cuts))
        loudness = loudness * jnp.repeat(jnp.exp(draws), extent[axis_at] // parts).reshape((-1,) + (1,) * (len(extent) - 1 - axis_at))
    return loudness


def normal_values(rng, dims, width, limit, cuts=(), held_as=jnp.bfloat16):
    result = jax.random.normal(rng, dims, jnp.float32) * width
    if len(cuts) > 0:
        result = level_of(rng, dims, cuts, -0.22, 0.18) * result
    return jnp.clip(result, min=-limit, max=limit).astype(held_as)


def setup_inputs(seed: int = 0) -> dict:
    arg_keys = jax.random.split(jax.random.key(seed), 10)
    token_ids = draw_token_ids(jax.random.fold_in(arg_keys[9], 71), 0)
    sensitivity = normal_values(arg_keys[1], (RESPONSES, BLOCK, D), 1.0, 6.0, ((0, 32),))
    last_hidden = normal_values(arg_keys[2], (RESPONSES, D), 1.0, 6.0, ((0, 32),))
    lengths = set_ends(jax.random.randint(arg_keys[3], (RESPONSES,), BLOCK - BLOCK // 4 + 1, BLOCK + 1), jax.random.fold_in(arg_keys[3], 1), BLOCK - BLOCK // 4 + 1, BLOCK).astype(jnp.int32)
    norm_gain = jnp.clip(1.0 + 0.15 * jax.random.normal(arg_keys[4], (D,), jnp.float32), 0.25, 1.75)
    reward_head = normal_values(arg_keys[5], (D,), D ** -0.5, 0.09375, (), jnp.float32)
    chosen_index = draw_chosen_index(jax.random.fold_in(arg_keys[9], 71), 0)
    rejected_index = draw_rejected_index(jax.random.fold_in(arg_keys[9], 71), 0)
    shard_owner = jax.random.permutation(arg_keys[8], DEVICES).astype(jnp.int32)
    return {"token_ids": token_ids, "sensitivity": sensitivity, "last_hidden": last_hidden, "lengths": lengths, "norm_gain": norm_gain, "reward_head": reward_head, "chosen_index": chosen_index, "rejected_index": rejected_index, "shard_owner": shard_owner}


def reference(token_ids, sensitivity, last_hidden, lengths, norm_gain, reward_head, chosen_index, rejected_index, shard_owner):
    hidden = last_hidden.astype(jnp.float32)
    normed = hidden / jnp.sqrt(lax.optimization_barrier(jnp.mean(hidden * hidden, axis=-1, keepdims=True)) + 1e-05) * norm_gain
    reward = lax.optimization_barrier(jnp.sum(normed * reward_head, axis=-1))
    margin = reward[chosen_index] - reward[rejected_index]
    push = -jax.nn.sigmoid(-margin)
    reward_grad = jnp.zeros((RESPONSES,), jnp.float32).at[chosen_index].add(push).at[rejected_index].add(-push)
    head_grad = lax.optimization_barrier(jnp.sum(reward_grad[:, None] * normed, axis=0))
    slots = jnp.arange(BLOCK, dtype=jnp.int32)
    live = slots[None, :] < lengths[:, None]
    scale_all = jnp.where(live, reward_grad[:, None], jnp.float32(0.0))
    ids_dev = token_ids.reshape(DEVICES, RESP_DEV * BLOCK)
    sens_dev = sensitivity.reshape(DEVICES, RESP_DEV * BLOCK, D)
    scale_dev = scale_all.reshape(DEVICES, RESP_DEV * BLOCK)

    def accumulate(table, items):
        ids, sens, scale = items
        rows = (scale[:, None] * sens.astype(jnp.float32)).astype(jnp.bfloat16)
        return (table.at[ids].add(rows.astype(jnp.float32)), None)
    table = jnp.zeros((VOCAB, D), jnp.float32)
    table, _ = lax.scan(accumulate, table, (ids_dev, sens_dev, scale_dev))
    inverse = jnp.argsort(shard_owner).astype(jnp.int32)
    owned = table.reshape(DEVICES, SHARD, D)[inverse].reshape(VOCAB, D)
    return (owned.astype(jnp.bfloat16), head_grad)
```

```python
import functools

import jax
import jax.numpy as jnp
from jax import lax
from jax.experimental import pallas as pl
from jax.experimental.pallas import tpu as pltpu
from jax.sharding import PartitionSpec as P

VOCAB = 128256
MESH = pl.DeviceIdType.MESH


def exchange_kernel(n, n_dev, meta_ref, rows_ref, meta_out, rows_out, send_sem, recv_sem, own_sem):
    me = lax.axis_index("grp") * n_dev + lax.axis_index("dev")

    def coord(t):
        return (t // n_dev, lax.rem(t, n_dev))

    barrier = pltpu.get_barrier_semaphore()

    def greet(k, c):
        t = lax.rem(me + k, n)
        pl.semaphore_signal(barrier, inc=1, device_id=coord(t), device_id_type=MESH)
        return c

    lax.fori_loop(1, n, greet, 0)
    own = [
        pltpu.make_async_copy(src.at[me], dst.at[me], own_sem.at[i])
        for i, (src, dst) in enumerate(((meta_ref, meta_out), (rows_ref, rows_out)))
    ]
    for c in own:
        c.start()
    pl.semaphore_wait(barrier, n - 1)

    def copies(src_block, dst_block, to):
        return [
            pltpu.make_async_remote_copy(
                src_ref=src.at[src_block],
                dst_ref=dst.at[dst_block],
                send_sem=send_sem.at[i, src_block],
                recv_sem=recv_sem.at[i, dst_block],
                device_id=coord(to),
                device_id_type=MESH,
            )
            for i, (src, dst) in enumerate(((meta_ref, meta_out), (rows_ref, rows_out)))
        ]

    def send(k, c):
        t = lax.rem(me + k, n)
        for cp in copies(t, me, t):
            cp.start()
        return c

    lax.fori_loop(1, n, send, 0)

    def finish(k, c):
        t = lax.rem(me + k, n)
        for cp in copies(t, me, t):
            cp.wait_send()
        s = lax.rem(me + n - k, n)
        for cp in copies(s, s, s):
            cp.wait_recv()
        return c

    lax.fori_loop(1, n, finish, 0)
    for c in own:
        c.wait()


def exchange(meta, rows, n, n_dev):
    anyspec = pl.BlockSpec(memory_space=pl.ANY)
    return pl.pallas_call(
        functools.partial(exchange_kernel, n, n_dev),
        out_shape=(
            jax.ShapeDtypeStruct(meta.shape, meta.dtype),
            jax.ShapeDtypeStruct(rows.shape, rows.dtype),
        ),
        in_specs=[anyspec, anyspec],
        out_specs=(anyspec, anyspec),
        scratch_shapes=[
            pltpu.SemaphoreType.DMA((2, n)),
            pltpu.SemaphoreType.DMA((2, n)),
            pltpu.SemaphoreType.DMA((2,)),
        ],
        compiler_params=pltpu.CompilerParams(collective_id=0, has_side_effects=True),
    )(meta, rows)


def local(
    token_ids,
    sensitivity,
    last_hidden,
    lengths,
    norm_gain,
    reward_head,
    chosen_index,
    rejected_index,
    shard_owner,
):
    resp_local, block_len = token_ids.shape
    width = sensitivity.shape[2]
    tok_local = resp_local * block_len
    n_dev = lax.axis_size("dev")
    devices = shard_owner.shape[0]
    responses = devices * resp_local
    shard_rows = VOCAB // devices
    capacity = max(2, (2 * tok_local + devices - 1) // devices)
    cols = width // devices
    lanes = -(-max(cols, capacity, resp_local) // 128) * 128
    hidden = last_hidden.astype(jnp.float32)
    normed = (
        hidden / jnp.sqrt(jnp.mean(hidden * hidden, axis=-1, keepdims=True) + 1e-05) * norm_gain
    )
    own_reward = jnp.sum(normed * reward_head, axis=-1)

    positions = jnp.arange(block_len, dtype=jnp.int32)
    live = (positions[None, :] < lengths[:, None]).reshape(tok_local)
    ids = token_ids.reshape(tok_local)
    shard_of = ids // shard_rows
    offset = ids - shard_of * shard_rows
    shard_hot = shard_of[:, None] == jnp.arange(devices, dtype=jnp.int32)[None, :]
    owner = jnp.sum(jnp.where(shard_hot, shard_owner[None, :], 0), axis=1)
    live_hot = (shard_hot & live[:, None]).astype(jnp.bfloat16)
    token_pos = jnp.arange(tok_local, dtype=jnp.int32)
    earlier = (token_pos[:, None] > token_pos[None, :]).astype(jnp.bfloat16)
    before = jnp.dot(earlier, live_hot, preferred_element_type=jnp.float32)
    rank = jnp.sum(before * live_hot.astype(jnp.float32), axis=1).astype(jnp.int32)
    slot = jnp.where(live, owner * capacity + rank, -1)
    slot_match = slot[None, :] == jnp.arange(devices * capacity, dtype=jnp.int32)[:, None]
    outgoing = jnp.dot(
        slot_match.astype(jnp.bfloat16),
        sensitivity.reshape(tok_local, width),
        preferred_element_type=jnp.float32,
    ).astype(jnp.bfloat16)
    code = (offset + 1) * resp_local + token_pos // block_len
    codes = jnp.sum(jnp.where(slot_match, code[None, :], 0), axis=1)
    codes = codes.reshape(devices, capacity)
    target_out = codes // resp_local - 1
    resp_out = codes - codes // resp_local * resp_local

    def lane_pad(a):
        return jnp.pad(a, ((0, 0), (0, lanes - a.shape[1])))[:, None, :]

    normed_blocks = normed.reshape(resp_local, devices, cols).transpose(1, 0, 2)
    meta = jnp.concatenate(
        [
            lane_pad(target_out.astype(jnp.float32)),
            lane_pad(resp_out.astype(jnp.float32)),
            lane_pad(jnp.broadcast_to(own_reward[None, :], (devices, resp_local))),
            jnp.zeros((devices, 1, lanes), jnp.float32),
            jnp.pad(normed_blocks, ((0, 0), (0, 0), (0, lanes - cols))),
        ],
        axis=1,
    )
    extra = -meta.shape[1] % 8
    meta = jnp.pad(meta, ((0, 0), (0, extra), (0, 0)))
    meta_in, arrived = exchange(
        meta, outgoing.reshape(devices, capacity, width), devices, n_dev
    )

    targets = meta_in[:, 0, :capacity].astype(jnp.int32).reshape(devices * capacity)
    resp_in = meta_in[:, 1, :capacity].astype(jnp.int32)
    reward = meta_in[:, 2, :resp_local].reshape(responses)
    normed_in = meta_in[:, 4 : 4 + resp_local, :cols]
    all_resp = jnp.arange(responses, dtype=jnp.int32)
    sign_table = (chosen_index[:, None] == all_resp[None, :]).astype(jnp.float32) - (
        rejected_index[:, None] == all_resp[None, :]
    ).astype(jnp.float32)
    margin = jnp.sum(sign_table * reward[None, :], axis=1)
    push = -jax.nn.sigmoid(-margin)
    reward_grad = jnp.sum(sign_table * push[:, None], axis=0).reshape(devices, resp_local)
    head_grad = jnp.sum(reward_grad[:, :, None] * normed_in, axis=(0, 1))
    resp_hot = resp_in[:, :, None] == jnp.arange(resp_local, dtype=jnp.int32)[None, None, :]
    scale = jnp.sum(jnp.where(resp_hot, reward_grad[:, None, :], 0.0), axis=2)
    scaled = (scale[:, :, None] * arrived).astype(jnp.bfloat16).reshape(devices * capacity, width)
    placing = (targets[None, :] == jnp.arange(shard_rows, dtype=jnp.int32)[:, None]).astype(
        jnp.bfloat16
    )
    owned = jnp.dot(placing, scaled, preferred_element_type=jnp.float32).astype(jnp.bfloat16)
    return (owned, head_grad)


def solution(mesh):
    placed = (
        P(("grp", "dev"), None),
        P(("grp", "dev"), None, None),
        P(("grp", "dev"), None),
        P(("grp", "dev")),
        P(),
        P(),
        P(),
        P(),
        P(),
    )
    return jax.shard_map(
        local,
        mesh=mesh,
        in_specs=placed,
        out_specs=(P(("grp", "dev"), None), P(("grp", "dev"))),
        check_vma=False,
    )
```

```python
import functools

import jax
import jax.numpy as jnp
from jax import lax
from jax.experimental import pallas as pl
from jax.experimental.pallas import tpu as pltpu
from jax.sharding import PartitionSpec as P

VOCAB = 128256
MESH = pl.DeviceIdType.MESH


def exchange_kernel(n, n_dev, meta_ref, rows_ref, meta_out, rows_out, send_sem, recv_sem, own_sem):
    me = lax.axis_index("grp") * n_dev + lax.axis_index("dev")

    def coord(t):
        return (t // n_dev, lax.rem(t, n_dev))

    barrier = pltpu.get_barrier_semaphore()

    def greet(k, c):
        t = lax.rem(me + k, n)
        pl.semaphore_signal(barrier, inc=1, device_id=coord(t), device_id_type=MESH)
        return c

    lax.fori_loop(1, n, greet, 0)
    own = [
        pltpu.make_async_copy(src.at[me], dst.at[me], own_sem.at[i])
        for i, (src, dst) in enumerate(((meta_ref, meta_out), (rows_ref, rows_out)))
    ]
    for c in own:
        c.start()
    pl.semaphore_wait(barrier, n - 1)

    def copies(src_block, dst_block, to):
        return [
            pltpu.make_async_remote_copy(
                src_ref=src.at[src_block],
                dst_ref=dst.at[dst_block],
                send_sem=send_sem.at[i, src_block],
                recv_sem=recv_sem.at[i, dst_block],
                device_id=coord(to),
                device_id_type=MESH,
            )
            for i, (src, dst) in enumerate(((meta_ref, meta_out), (rows_ref, rows_out)))
        ]

    def send(k, c):
        t = lax.rem(me + k, n)
        for cp in copies(t, me, t):
            cp.start()
        return c

    lax.fori_loop(1, n, send, 0)

    def finish(k, c):
        t = lax.rem(me + k, n)
        for cp in copies(t, me, t):
            cp.wait_send()
        s = lax.rem(me + n - k, n)
        for cp in copies(s, s, s):
            cp.wait_recv()
        return c

    lax.fori_loop(1, n, finish, 0)
    for c in own:
        c.wait()


def exchange(meta, rows, n, n_dev):
    anyspec = pl.BlockSpec(memory_space=pl.ANY)
    return pl.pallas_call(
        functools.partial(exchange_kernel, n, n_dev),
        out_shape=(
            jax.ShapeDtypeStruct(meta.shape, meta.dtype),
            jax.ShapeDtypeStruct(rows.shape, rows.dtype),
        ),
        in_specs=[anyspec, anyspec],
        out_specs=(anyspec, anyspec),
        scratch_shapes=[
            pltpu.SemaphoreType.DMA((2, n)),
            pltpu.SemaphoreType.DMA((2, n)),
            pltpu.SemaphoreType.DMA((2,)),
        ],
        compiler_params=pltpu.CompilerParams(collective_id=0, has_side_effects=True),
    )(meta, rows)


def local(
    token_ids,
    sensitivity,
    last_hidden,
    lengths,
    norm_gain,
    reward_head,
    chosen_index,
    rejected_index,
    shard_owner,
):
    resp_local, block_len = token_ids.shape
    width = sensitivity.shape[2]
    tok_local = resp_local * block_len
    n_dev = lax.axis_size("dev")
    devices = shard_owner.shape[0]
    responses = devices * resp_local
    shard_rows = VOCAB // devices
    capacity = max(2, (2 * tok_local + devices - 1) // devices)
    cols = width // devices
    lanes = -(-max(cols, capacity, resp_local) // 128) * 128
    hidden = last_hidden.astype(jnp.float32)
    normed = (
        hidden / jnp.sqrt(jnp.mean(hidden * hidden, axis=-1, keepdims=True) + 1e-05) * norm_gain
    )
    own_reward = jnp.sum(normed * reward_head, axis=-1)

    positions = jnp.arange(block_len, dtype=jnp.int32)
    live = (positions[None, :] < lengths[:, None]).reshape(tok_local)
    ids = token_ids.reshape(tok_local)
    shard_of = ids // shard_rows
    offset = ids - shard_of * shard_rows
    shard_hot = shard_of[:, None] == jnp.arange(devices, dtype=jnp.int32)[None, :]
    owner = jnp.sum(jnp.where(shard_hot, shard_owner[None, :], 0), axis=1)
    live_hot = (shard_hot & live[:, None]).astype(jnp.bfloat16)
    token_pos = jnp.arange(tok_local, dtype=jnp.int32)
    earlier = (token_pos[:, None] > token_pos[None, :]).astype(jnp.bfloat16)
    before = jnp.dot(earlier, live_hot, preferred_element_type=jnp.float32)
    rank = jnp.sum(before * live_hot.astype(jnp.float32), axis=1).astype(jnp.int32)
    slot = jnp.where(live, owner * capacity + rank, -1)
    slot_match = slot[None, :] == jnp.arange(devices * capacity, dtype=jnp.int32)[:, None]
    outgoing = jnp.dot(
        slot_match.astype(jnp.bfloat16),
        sensitivity.reshape(tok_local, width),
        preferred_element_type=jnp.float32,
    ).astype(jnp.bfloat16)
    code = (offset + 1) * resp_local + token_pos // block_len
    codes = jnp.sum(jnp.where(slot_match, code[None, :], 0), axis=1)
    codes = codes.reshape(devices, capacity)
    target_out = codes // resp_local - 1
    resp_out = codes - codes // resp_local * resp_local

    def lane_pad(a):
        return jnp.pad(a, ((0, 0), (0, lanes - a.shape[1])))[:, None, :]

    normed_blocks = normed.reshape(resp_local, devices, cols).transpose(1, 0, 2)
    meta = jnp.concatenate(
        [
            lane_pad(target_out.astype(jnp.float32)),
            lane_pad(resp_out.astype(jnp.float32)),
            lane_pad(jnp.broadcast_to(own_reward[None, :], (devices, resp_local))),
            jnp.zeros((devices, 1, lanes), jnp.float32),
            jnp.pad(normed_blocks, ((0, 0), (0, 0), (0, lanes - cols))),
        ],
        axis=1,
    )
    extra = -meta.shape[1] % 8
    meta = jnp.pad(meta, ((0, 0), (0, extra), (0, 0)))
    meta_in, arrived = exchange(
        meta, outgoing.reshape(devices, capacity, width), devices, n_dev
    )

    targets = meta_in[:, 0, :capacity].astype(jnp.int32).reshape(devices * capacity)
    resp_in = meta_in[:, 1, :capacity].astype(jnp.int32)
    reward = meta_in[:, 2, :resp_local].reshape(responses)
    normed_in = meta_in[:, 4 : 4 + resp_local, :cols]
    all_resp = jnp.arange(responses, dtype=jnp.int32)
    sign_table = (chosen_index[:, None] == all_resp[None, :]).astype(jnp.float32) - (
        rejected_index[:, None] == all_resp[None, :]
    ).astype(jnp.float32)
    margin = jnp.sum(sign_table * reward[None, :], axis=1)
    push = -jax.nn.sigmoid(-margin)
    reward_grad = jnp.sum(sign_table * push[:, None], axis=0).reshape(devices, resp_local)
    head_grad = jnp.sum(reward_grad[:, :, None] * normed_in, axis=(0, 1))
    resp_hot = resp_in[:, :, None] == jnp.arange(resp_local, dtype=jnp.int32)[None, None, :]
    scale = jnp.sum(jnp.where(resp_hot, reward_grad[:, None, :], 0.0), axis=2)
    total = devices * capacity
    scale = scale.reshape(total)
    rows_in = arrived.reshape(total, width)

    def place_all(operands):
        rows, targets, scale = operands
        scaled = (scale[:, None] * rows).astype(jnp.bfloat16)
        placing = (targets[None, :] == jnp.arange(shard_rows, dtype=jnp.int32)[:, None]).astype(
            jnp.bfloat16
        )
        return jnp.dot(placing, scaled, preferred_element_type=jnp.float32).astype(jnp.bfloat16)

    operands = (rows_in, targets, scale)
    blocks, window = 3, total // 4
    if shard_rows % (8 * blocks) or window % 128:
        owned = place_all(operands)
        return (owned, head_grad)
    block_rows = shard_rows // blocks
    first_row = jnp.arange(blocks, dtype=jnp.int32) * block_rows
    in_block = (targets[:, None] >= first_row[None, :]) & (
        targets[:, None] < first_row[None, :] + block_rows
    )
    block_hot = in_block.astype(jnp.bfloat16)
    pos = jnp.arange(total, dtype=jnp.int32)
    ahead = (pos[:, None] > pos[None, :]).astype(jnp.bfloat16)
    rank_in = jnp.dot(ahead, block_hot, preferred_element_type=jnp.float32).astype(jnp.int32)
    slot_base = jnp.arange(blocks, dtype=jnp.int32) * window
    packed_slot = jnp.sum(jnp.where(in_block, rank_in + slot_base[None, :] + 1, 0), axis=1) - 1
    fits = jnp.max(jnp.sum(in_block.astype(jnp.int32), axis=0)) <= window

    def place_packed(operands):
        rows, targets, scale = operands
        pack = packed_slot[None, :] == jnp.arange(blocks * window, dtype=jnp.int32)[:, None]
        packed_scale = jnp.sum(jnp.where(pack, scale[None, :], 0.0), axis=1)
        packed_target = jnp.sum(jnp.where(pack, targets[None, :] + 1, 0), axis=1) - 1
        packed = jnp.dot(pack.astype(jnp.bfloat16), rows, preferred_element_type=jnp.float32)
        packed = (packed_scale[:, None] * packed).astype(jnp.bfloat16)
        row_of = first_row[:, None] + jnp.arange(block_rows, dtype=jnp.int32)[None, :]
        placing = packed_target.reshape(blocks, 1, window) == row_of[:, :, None]
        owned = lax.dot_general(
            placing.astype(jnp.bfloat16),
            packed.reshape(blocks, window, width),
            (((2,), (1,)), ((0,), (0,))),
            preferred_element_type=jnp.float32,
        )
        return owned.astype(jnp.bfloat16).reshape(shard_rows, width)

    owned = lax.cond(fits, place_packed, place_all, operands)
    return (owned, head_grad)


def solution(mesh):
    placed = (
        P(("grp", "dev"), None),
        P(("grp", "dev"), None, None),
        P(("grp", "dev"), None),
        P(("grp", "dev")),
        P(),
        P(),
        P(),
        P(),
        P(),
    )
    return jax.shard_map(
        local,
        mesh=mesh,
        in_specs=placed,
        out_specs=(P(("grp", "dev"), None), P(("grp", "dev"))),
        check_vma=False,
    )
```
